256 devices in a mesh: row: 8 (over z_hi, x), col: 32 (over z_lo, y, core).
Axes of the slice: x: 4, y: 4, z: 8 (z_hi: 2, z_lo: 4; z = z_hi * 4 + z_lo), core: 2. Of those that a mesh axis runs over, the one named last changes fastest.
Arguments:
- matrix: bfloat16 [3072, 262144], P('row', 'col'), may hold values from -0.01171875 to 0.01171875
- probes: bfloat16 [262144, 128], P('col'), may hold values from -6 to 6
Outputs:
- krylov: bfloat16 [2, 262144, 128], P(None, 'col')
The draws below stay inside these ranges and needn't reach their ends.
All inputs are finite; a program needn't handle non-finite values.
Results may differ from the reference program's by a relative error of at most 0.0054.
Values may be sent and summed in bfloat16 or wider, within the bound.
No kernel may reach another device: no remote copies, remote signals or barrier semaphores. Data moves between devices by JAX's collectives and lax.ppermute only.
A program may use at most 64 MiB of HBM per device.

```python
import math
import jax
import jax.numpy as jnp
from jax import lax

N = 262144
K = 128
ITERS = 2
M = 3072


def level_of(own_key, extent, split, smallest, largest):
    gain, own = 1.0, jax.random.fold_in(own_key, 6)
    for axis_at, shards_of in split:
        draws = jnp.exp(jax.random.uniform(jax.random.fold_in(own, axis_at), (shards_of,), jnp.float32, smallest / len(split), largest / len(split)))
        gain = gain * jnp.repeat(draws, extent[axis_at] // shards_of).reshape([-1 if axis == axis_at else 1 for axis in range(len(extent))])
    return gain


def bell_draw(own_key, extent, scale, limit, pieces=(), kind=jnp.bfloat16):
    result = jax.random.normal(own_key, extent, jnp.float32) * scale
    if len(pieces) > 0:
        result = level_of(own_key, extent, pieces, -0.22, 0.18) * result
    return jnp.clip(result, min=-limit, max=limit).astype(kind)


def setup_inputs(seed: int = 0) -> dict:
    streams_of = jax.random.split(jax.random.key(seed), 3)
    return {
        "matrix": bell_draw(streams_of[0], (M, N), N ** -0.5, 0.01171875, ((0, 8), (1, 32))),
        "probes": bell_draw(streams_of[1], (N, K), 1.0, 6.0, ((0, 32),)),
    }


def reference(matrix, probes):
    stretch = math.sqrt(N / M)
    current = probes
    results = []
    for level in range(ITERS):
        factor = 1.0 if level == 0 else 1.0 / stretch
        partial_value = jnp.dot(matrix, current, preferred_element_type=jnp.float32)
        reduced = (partial_value * factor).astype(jnp.bfloat16)
        back = lax.dot_general(matrix, reduced, (((0,), (0,)), ((), ())), preferred_element_type=jnp.float32)
        current = (back * stretch).astype(jnp.bfloat16)
        results.append(current)
    return jnp.stack(results)
```

```python
import functools
import math

import jax
import jax.numpy as jnp
from jax import lax
from jax.experimental import pallas as pl
from jax.experimental.pallas import tpu as pltpu
from jax.sharding import Mesh
from jax.sharding import PartitionSpec as P

ITERS = 2
CHUNKS = 2

FIRST = ((2, 0), (1, 1), (2, 1), (3, 0))
LATER = ((1, 0), (3, 1), (0, 0), (0, 1))


def shifted(value, axis, step):
    length = lax.axis_size(axis)
    return lax.ppermute(value, axis, [(i, (i + step) % length) for i in range(length)])


def pick(options, at):
    chosen = options[-1]
    for i in range(len(options) - 2, -1, -1):
        chosen = jnp.where(at == i, options[i], chosen)
    return chosen


def back_kernel(count, x_ref, z_ref, a_ref, left_ref, right_ref, turned):
    step = pl.program_id(0)

    @pl.when(step == 0)
    def _():
        turned[...] = z_ref[...].T

    part = jnp.dot(turned[...], a_ref[...], preferred_element_type=jnp.float32).T
    half = part.shape[0]
    for i in range(count):
        out = left_ref if i < count // 2 else right_ref
        at = (i % (count // 2)) * half

        @pl.when(step == i)
        def _():
            out[at : at + half, :] = part.astype(out.dtype)


def back_pieces(place, z, matrix, pieces, chunk, half, kinds):
    rows, columns = matrix.shape
    width = z.shape[1]
    per_slice = columns // half // 4
    count = len(pieces)

    def column(i, place):
        offset = pick([jnp.int32(p[0]) for p in pieces], i)
        inner = pick([jnp.int32(p[1]) for p in pieces], i)
        return 0, lax.rem(place[0] + offset, 4) * per_slice + 2 * chunk + inner

    size = (count // 2) * half
    whole = pl.BlockSpec((size, width), lambda i, place: (0, 0))
    return pl.pallas_call(
        functools.partial(back_kernel, count),
        out_shape=[jax.ShapeDtypeStruct((size, width), kind) for kind in kinds],
        grid_spec=pltpu.PrefetchScalarGridSpec(
            num_scalar_prefetch=1,
            grid=(count,),
            in_specs=[
                pl.BlockSpec((rows, width), lambda i, place: (0, 0)),
                pl.BlockSpec((rows, half), column),
            ],
            out_specs=[whole, whole],
            scratch_shapes=[pltpu.VMEM((width, rows), z.dtype)],
        ),
        cost_estimate=pl.CostEstimate(
            flops=2 * rows * width * half * count, bytes_accessed=2 * rows * half * count, transcendentals=0
        ),
        name="back",
    )(place, z, matrix)


def forward_kernel(x_ref, a_ref, own, left, right, far_a, far_b, acc_ref, *refs):
    acc_out, out_ref = refs[-2:]
    step = pl.program_id(0)

    @pl.when(step == 0)
    def _():
        acc_out[...] = acc_ref[...]

    for i, piece in enumerate((own, left, right)):

        @pl.when(step == i)
        def _():
            out_ref[0] = piece[...]

    @pl.when(step == 3)
    def _():
        out_ref[0] = jnp.concatenate([far_a[...], far_b[...]], axis=0)

    acc_out[...] += jnp.dot(a_ref[...], out_ref[0], preferred_element_type=jnp.float32)


def place_kernel(x_ref, own, left, right, far_a, far_b, *refs):
    out_ref = refs[-1]
    step = pl.program_id(0)
    for i, piece in enumerate((own, left, right)):

        @pl.when(step == i)
        def _():
            out_ref[0] = piece[...]

    @pl.when(step == 3)
    def _():
        out_ref[0] = jnp.concatenate([far_a[...], far_b[...]], axis=0)


def slice_of(step, place):
    return lax.rem(place[0] + pick([jnp.int32(o) for o in (0, 3, 1, 2)], step), 4)


def forward_pieces(place, matrix, pieces, acc, out, level, chunk, chunks):
    rows = matrix.shape[0]
    length, width = pieces[0].shape

    def at(i, place):
        return slice_of(i, place) * chunks + chunk

    whole = lambda value: pl.BlockSpec(value.shape, lambda i, place: (0, 0))
    placed = pl.BlockSpec((1, length, width), lambda i, place: (level, at(i, place), 0))
    block = pl.BlockSpec((rows, length), lambda i, place: (0, at(i, place)))
    made = jax.ShapeDtypeStruct((ITERS, matrix.shape[1], width), jnp.bfloat16)
    kept = () if out is None else (out,)
    aliased = [pl.BlockSpec(memory_space=pl.ANY)] * len(kept)
    if acc is None:
        return None, pl.pallas_call(
            place_kernel,
            out_shape=made,
            grid_spec=pltpu.PrefetchScalarGridSpec(
                num_scalar_prefetch=1,
                grid=(4,),
                in_specs=[*(whole(p) for p in pieces), *aliased],
                out_specs=placed,
            ),
            input_output_aliases={6: 0} if kept else {},
            name="place",
        )(place, *pieces, *kept)
    return pl.pallas_call(
        forward_kernel,
        out_shape=[jax.ShapeDtypeStruct(acc.shape, acc.dtype), made],
        grid_spec=pltpu.PrefetchScalarGridSpec(
            num_scalar_prefetch=1,
            grid=(4,),
            in_specs=[block, *(whole(p) for p in pieces), whole(acc), *aliased],
            out_specs=[whole(acc), placed],
        ),
        input_output_aliases={8: 1} if kept else {},
        cost_estimate=pl.CostEstimate(
            flops=8 * rows * width * length, bytes_accessed=8 * rows * length, transcendentals=0
        ),
        name="forward",
    )(place, matrix, *pieces, acc, *kept)


def exchanged_sum(value, axis):
    length = lax.axis_size(axis)
    return sum((shifted(value, axis, k) for k in range(1, length)), value)


def scattered_sum(value, axis):
    length = lax.axis_size(axis)
    me = lax.axis_index(axis)
    size = value.shape[0] // length
    part = lambda k: lax.dynamic_slice_in_dim(value, lax.rem(me + k, length) * size, size, 0)
    return sum((shifted(part(k), axis, k) for k in range(1, length)), part(0))


def gathered(value, axis):
    length = lax.axis_size(axis)
    me = lax.axis_index(axis)
    size = value.shape[0]
    whole = jnp.zeros((size * length, value.shape[1]), value.dtype)
    for k in range(length):
        piece = value if k == 0 else shifted(value, axis, k)
        at = lax.rem(me + length - k, length) * size
        whole = lax.dynamic_update_slice_in_dim(whole, piece, at, 0)
    return whole


def column_sum(partial_value, factor):
    value = scattered_sum(partial_value, "core")
    value = scattered_sum(value, "y")
    value = exchanged_sum(value, "z_lo")
    value = (value * factor).astype(jnp.bfloat16)
    return gathered(gathered(value, "y"), "core")


def chunk_sum(place, z, matrix, chunk, half, stretch):
    single = jnp.float32
    plus, minus = back_pieces(place, z, matrix, FIRST, chunk, half, (jnp.bfloat16, jnp.bfloat16))
    got_plus, got_minus = shifted(plus, "x", 1), shifted(minus, "x", -1)
    relay, own = back_pieces(place, z, matrix, LATER, chunk, half, (jnp.bfloat16, single))
    onward_plus = (relay[:half].astype(single) + got_plus[:half]).astype(jnp.bfloat16)
    onward_minus = (relay[half:].astype(single) + got_minus[:half]).astype(jnp.bfloat16)
    got_onward_plus, got_onward_minus = shifted(onward_plus, "x", 1), shifted(onward_minus, "x", -1)
    summed = jnp.concatenate(
        [
            own[:half] + got_onward_plus + got_minus[half:],
            own[half:] + got_plus[half:] + got_onward_minus,
        ],
        axis=0,
    ).astype(jnp.bfloat16)
    other = shifted(summed, "z_hi", 1)
    return ((summed.astype(single) + other) * stretch).astype(jnp.bfloat16)


def spread(value, half):
    left, right = shifted(value, "x", 1), shifted(value, "x", -1)
    far_a, far_b = shifted(left[:half], "x", 1), shifted(right[half:], "x", -1)
    return value, left, right, far_a, far_b


def body(matrix, probes):
    rows, columns = matrix.shape
    width = probes.shape[1]
    m_total = rows * lax.axis_size(("z_hi", "x"))
    n_total = columns * lax.axis_size(("z_lo", "y", "core"))
    stretch = math.sqrt(n_total / m_total)
    half = columns // 4 // CHUNKS // 2
    place = lax.axis_index("x").astype(jnp.int32).reshape(1)
    partial_value = jnp.dot(matrix, probes, preferred_element_type=jnp.float32)
    out = None
    for level in range(ITERS):
        z = column_sum(partial_value, 1.0 if level == 0 else 1.0 / stretch)
        acc = None if level == ITERS - 1 else jnp.zeros((rows, width), jnp.float32)
        for chunk in range(CHUNKS):
            value = chunk_sum(place, z, matrix, chunk, half, stretch)
            pieces = spread(value, half)
            acc, out = forward_pieces(place, matrix, pieces, acc, out, level, chunk, CHUNKS)
        partial_value = acc
    return out


def solution(mesh):
    sizes = (2, 4, 4, 4, 2)
    torus = Mesh(mesh.devices.reshape(sizes), ("z_hi", "x", "z_lo", "y", "core"))
    row, col = ("z_hi", "x"), ("z_lo", "y", "core")
    placed = (P(row, col), P(col, None))
    return jax.shard_map(
        body, mesh=torus, in_specs=placed, out_specs=P(None, col, None), check_vma=False
    )
```

```python
import functools
import math

import jax
import jax.numpy as jnp
from jax import lax
from jax.experimental import pallas as pl
from jax.experimental.pallas import tpu as pltpu
from jax.sharding import Mesh
from jax.sharding import PartitionSpec as P


ITERS = 2
SIXTEENTHS = (5, 6, 5)
STEPS = ((1, 2), (1, 1), (2, 1))
TURNS = (
    "B1 Da0 B3 Dn0",
    "Df0 Df1 B2 Da1",
    "Dn1 T0 M2 T1",
    "R2 A0 T2 J0",
    "Ea1 Ef1 En1 F0",
    "Ea2 Ef2 En2 F1",
    "F2",
)
TURNS = tuple(turn for group in TURNS for turn in group.split())
PARAMS = pltpu.CompilerParams(vmem_limit_bytes=12 * 2**20)
VMEM = pl.BlockSpec(memory_space=pltpu.VMEM)
SMEM = pl.BlockSpec(memory_space=pltpu.SMEM)
HBM = pl.BlockSpec(memory_space=pltpu.HBM)
SINGLE = jnp.float32
SHORT = jnp.bfloat16


def shaped(rows, like, kind):
    return jax.ShapeDtypeStruct((rows, like.shape[-1]), kind)


def call(kernel, outs, ins, specs, out_specs, flops=0, scratch=(), alias=None, params=PARAMS):
    moved = sum(math.prod(o.shape) * o.dtype.itemsize for o in outs)
    return pl.pallas_call(
        kernel,
        out_shape=outs,
        in_specs=specs,
        out_specs=out_specs,
        scratch_shapes=scratch,
        input_output_aliases=alias or {},
        compiler_params=params,
        cost_estimate=pl.CostEstimate(
            flops=flops + 4 * moved, bytes_accessed=moved, transcendentals=0
        ),
    )(*ins)


def split_by_core(total, core, mine, other):
    half = total.shape[0] // 2
    top, bottom = total[:half], total[half:]
    mine[...] = jnp.where(core == 0, top, bottom)
    other[...] = jnp.where(core == 0, bottom, top)


def first_kernel(core_ref, x_index_ref, a_ref, x_ref, mine, other):
    total = jnp.dot(a_ref[...], x_ref[...], preferred_element_type=SINGLE)
    split_by_core(total, core_ref[0], mine, other)


def first_product(core, x, matrix, probes):
    rows, columns = matrix.shape
    part = shaped(rows // 2, probes, SINGLE)
    return call(
        first_kernel,
        [part, part],
        (core, x, matrix, probes),
        [SMEM, SMEM, VMEM, VMEM],
        [VMEM, VMEM],
        2 * rows * columns * probes.shape[1],
    )


def columns_of(place, piece, block):
    stride, start, size = block
    x, core = place
    flip, across = jnp.bitwise_xor(x, 1), 3 - x
    owner = (
        x,
        jnp.where(core == 0, across, flip),
        jnp.where(core == 0, flip, across),
        jnp.bitwise_xor(x, 2),
    )[piece]
    return pl.ds(pl.multiple_of(owner * stride + start, 128), size)


def back_kernel(plan, x_ref, core_ref, mine, other, a_ref, *outs):
    core = core_ref[0]
    place = x_ref[0], core
    top = jnp.where(core == 0, mine[...], other[...])
    bottom = jnp.where(core == 0, other[...], mine[...])
    turned = jnp.concatenate([top, bottom], axis=0).T
    for out, (pieces, block, _) in zip(outs, plan):
        size = block[2]
        for i, piece in enumerate(pieces):
            columns = a_ref[:, columns_of(place, piece, block)]
            part = jnp.dot(turned, columns, preferred_element_type=SINGLE).T
            out[i * size : (i + 1) * size] = part.astype(out.dtype)


def back_product(x, core, mine, other, matrix, plan):
    outs = [shaped(len(pieces) * block[2], mine, kind) for pieces, block, kind in plan]
    return call(
        functools.partial(back_kernel, plan),
        outs,
        (x, core, mine, other, matrix),
        [SMEM, SMEM, VMEM, VMEM, VMEM],
        [VMEM] * len(outs),
        matrix.shape[0] * matrix.shape[1] * mine.shape[1],
    )


def relay_kernel(near, got, out):
    size = near.shape[0]
    out[...] = (near[...] + got[size:].astype(SINGLE)).astype(out.dtype)


def total_kernel(*refs):
    *ins, out = refs
    size = out.shape[0]
    total = ins[0][...]
    for term in ins[1:]:
        total += term[:size].astype(SINGLE)
    out[...] = total.astype(out.dtype)


def scaled_kernel(scale, one, two, out):
    out[...] = ((one[...].astype(SINGLE) + two[...].astype(SINGLE)) * scale).astype(out.dtype)


def join_kernel(one, two, out):
    size = one.shape[0]
    out[:size] = one[...]
    out[size:] = two[...]


def small(kernel, rows, kind, *ins):
    return call(kernel, [shaped(rows, ins[0], kind)], ins, [VMEM] * len(ins), [VMEM])[0]


def forward_kernel(level, block, last, count, has_acc, has_out, x_ref, core_ref, *refs):
    place = x_ref[0], core_ref[0]
    given, refs = refs[:count], refs[count:]
    size = block[2]
    pieces = [ref.at[pl.ds(at, size)] for ref in given for at in range(0, ref.shape[0], size)]
    a_ref = acc_ref = None
    multiply = level < ITERS - 1
    if multiply:
        a_ref, refs = refs[0], refs[1:]
    if has_acc:
        acc_ref, refs = refs[0], refs[1:]
    if has_out:
        refs = refs[1:]
    out_ref, sems = refs[0], refs[-1]
    copies = [
        pltpu.make_async_copy(
            piece, out_ref.at[level, columns_of(place, i, block)], sems.at[i]
        )
        for i, piece in enumerate(pieces)
    ]
    for copy in copies:
        copy.start()
    if multiply:
        half = a_ref.shape[0] // 2
        core = core_ref[0]

        def rows_of(i, kept_sum):
            rows = pl.ds(pl.multiple_of(jnp.where(core == i, 0, half), half), half)
            total = jnp.zeros((half, given[0].shape[1]), SINGLE) if acc_ref is None else acc_ref[i]
            for k, piece in enumerate(pieces):
                columns = a_ref[rows, columns_of(place, k, block)]
                total += jnp.dot(columns, piece[...], preferred_element_type=SINGLE)
            kept_sum[...] = total

        if last:
            rows_of(0, refs[1])
            rows_of(1, refs[2])
        else:

            @pl.loop(0, 2)
            def _(i):
                rows_of(i, refs[1].at[i])

    for copy in copies:
        copy.wait()


def forward(x, core, matrix, pieces, acc, out, level, block, last):
    rows, columns = matrix.shape
    like = pieces[0]
    ins, specs = [x, core, *pieces], [SMEM, SMEM] + [VMEM] * len(pieces)
    outs, out_specs = [jax.ShapeDtypeStruct((ITERS, columns, like.shape[1]), SHORT)], [HBM]
    alias = {}
    if level < ITERS - 1:
        ins.append(matrix)
        specs.append(VMEM)
        part = shaped(rows // 2, like, SINGLE)
        both = jax.ShapeDtypeStruct((2, *part.shape), SINGLE)
        outs += [part, part] if last else [both]
        out_specs += [VMEM] * (len(outs) - 1)
    if acc is not None:
        ins.append(acc)
        specs.append(VMEM)
    if out is not None:
        alias = {len(ins): 0}
        ins.append(out)
        specs.append(HBM)
    kernel = functools.partial(
        forward_kernel, level, block, last, len(pieces), acc is not None, out is not None
    )
    return call(
        kernel,
        outs,
        ins,
        specs,
        out_specs,
        8 * rows * like.shape[1] * block[2],
        [pltpu.SemaphoreType.DMA((4,))],
        alias,
    )


def permuted(value, axes, partner):
    sizes = [lax.axis_size(a) for a in axes]
    pairs = []
    for i in range(math.prod(sizes)):
        at, rest = [], i
        for size in reversed(sizes):
            at.append(rest % size)
            rest //= size
        target = 0
        for size, coordinate in zip(sizes, partner(*reversed(at))):
            target = target * size + coordinate
        pairs.append((i, target))
    return lax.ppermute(value, axes, pairs)


def near_partner(at, core):
    return at ^ 1 if core == 0 else 3 - at


def far_partner(at, core):
    return at ^ 1 if core == 1 else 3 - at


def swap(value, axis, partner):
    return permuted(value, (axis, "core"), lambda at, core: (partner(at, core), core))


def other_core(value):
    return permuted(value, ("core",), lambda core: (1 - core,))


def sum_kernel(one, two, *refs):
    out = refs[-1]
    out[...] = one[...] + two[...]


def all_kernel(*refs):
    one, two, three, four, out = refs
    out[...] = (one[...] + two[...]) + (three[...] + four[...])


def round_kernel(factor, one, two, *refs):
    out = refs[-1]
    out[...] = ((one[...] + two[...]) * factor).astype(out.dtype)


def column_sum(mine, other, matrix, factor):
    def plus(kernel, kind, one, two, *more):
        outs = [jax.ShapeDtypeStruct(one.shape, kind)]
        ins = (one, two, *more)
        return call(kernel, outs, ins, [VMEM] * len(ins), [VMEM])[0]

    value = plus(sum_kernel, SINGLE, mine, other_core(other))
    across = permuted(value, ("y",), lambda at: (at ^ 2,))
    near = swap(value, "y", near_partner)
    far = swap(value, "y", far_partner)
    value = plus(all_kernel, SINGLE, value, near, far, across)
    step = swap(value, "z_lo", lambda at, core: at ^ (1 + core))
    value = plus(sum_kernel, SINGLE, value, step, matrix)
    step = swap(value, "z_lo", lambda at, core: at ^ (2 - core))
    value = plus(functools.partial(round_kernel, factor), SHORT, value, step, matrix)
    return value, other_core(value)


def body(matrix, probes):
    rows, columns = matrix.shape
    stretch = math.sqrt(
        columns * lax.axis_size(("z_lo", "y", "core")) / (rows * lax.axis_size(("z_hi", "x")))
    )
    x = lax.axis_index("x").astype(jnp.int32).reshape(1)
    core = lax.axis_index("core").astype(jnp.int32).reshape(1)
    mine, other = first_product(core, x, matrix, probes)
    out = None
    for level in range(ITERS):
        factor = 1.0 if level == 0 else 1.0 / stretch
        mine, other = column_sum(mine, other, matrix, factor)
        out, *results = rows_step(x, core, matrix, mine, other, out, level, stretch)
        if level < ITERS - 1:
            mine, other = results
    return out


def across_x(value):
    return permuted(value, ("x",), lambda at: (at ^ 2,))


MOVES = {
    "M": lambda v: swap(v, "x", near_partner),
    "R": lambda v: swap(v, "x", far_partner),
    "T": lambda v: permuted(v, ("z_hi",), lambda at: (1 - at,)),
    "A": lambda v: swap(v, "x", far_partner),
    "J": lambda v: swap(v, "x", near_partner),
    "n": lambda v: swap(v, "x", near_partner),
    "f": lambda v: swap(v, "x", far_partner),
    "a": across_x,
}
DIRECT = {"n": 2, "f": 1, "a": 3}


def rows_step(x, core, matrix, mine, other, out, level, stretch):
    slice_rows = matrix.shape[1] // 4
    sizes = [slice_rows * part // sum(SIXTEENTHS) for part in SIXTEENTHS]
    blocks = [(slice_rows, sum(sizes[:k]), size) for k, size in enumerate(sizes)]
    made, got, acc, results = {}, {}, None, ()
    for turn in TURNS:
        name, k = turn[:-1], int(turn[-1])
        if name == "B":
            plan, names = [], []
            for i, (block, steps) in enumerate(zip(blocks, STEPS)):
                if k != 2 and (i == 0) != (k == 1):
                    continue
                if k != 2 and steps[0] == 2:
                    plan.append(((2, 3), block, SHORT))
                    names.append(f"M{i}")
                elif k != 2:
                    plan += [((DIRECT[d],), block, SHORT) for d in "anf"]
                    names += [f"D{d}{i}" for d in "anf"]
                else:
                    plan.append(((0,), block, SINGLE))
                    names.append(f"own{i}")
                    if steps[0] == 2:
                        plan.append(((1,), block, SINGLE))
                        names.append(f"near{i}")
            made.update(zip(names, back_product(x, core, mine, other, matrix, tuple(plan))))
        elif name == "R":
            made[turn] = small(relay_kernel, sizes[k], SHORT, made[f"near{k}"], got[f"M{k}"])
        elif name == "T":
            froms = ("M", "R") if STEPS[k][0] == 2 else ("Da", "Dn", "Df")
            terms = [got[f"{f}{k}"] for f in froms]
            made[turn] = small(total_kernel, sizes[k], SHORT, made[f"own{k}"], *terms)
        elif name in ("A", "Ea"):
            kernel = functools.partial(scaled_kernel, stretch)
            value = small(kernel, sizes[k], SHORT, made[f"T{k}"], got[f"T{k}"])
            made.update({turn: value, f"En{k}": value, f"Ef{k}": value})
        elif name == "J":
            made[turn] = small(join_kernel, 2 * sizes[k], SHORT, made[f"A{k}"], got[f"A{k}"])
        elif name == "F":
            if STEPS[k][1] == 2:
                pieces = [made[f"J{k}"], got[f"J{k}"]]
            else:
                pieces = [made[f"Ea{k}"], *(got[f"E{d}{k}"] for d in "fna")]
            last = k == len(sizes) - 1
            out, *results = forward(
                x, core, matrix, pieces, acc, out, level, blocks[k], last
            )
            acc = results[0] if results else None
        if name[-1] in MOVES:
            got[turn] = MOVES[name[-1]](made[turn])
    return out, *results


def solution(mesh):
    sizes = (2, 4, 4, 4, 2)
    torus = Mesh(mesh.devices.reshape(sizes), ("z_hi", "x", "z_lo", "y", "core"))
    row, col = ("z_hi", "x"), ("z_lo", "y", "core")
    placed = (P(row, col), P(col, None))
    return jax.shard_map(
        body, mesh=torus, in_specs=placed, out_specs=P(None, col, None), check_vma=False
    )
```
